32 devices in a mesh: dp: 8 (over z, y), expert: 4 (over x, core).
Axes of the slice: x: 2, y: 2, z: 4, core: 2. Of those that a mesh axis runs over, the one named last changes fastest.
Arguments:
- queries: bfloat16 [4096, 4096], P('dp', 'expert'), may hold values from -6 to 6
- key_states: bfloat16 [4096, 4096], P('dp', 'expert'), may hold values from -6 to 6
- value_states: bfloat16 [4096, 4096], P('dp', 'expert'), may hold values from -6 to 6
- doc_lengths: int32 [8, 8], replicated, may hold values from 0 to 512, as said below
- move_plan: int32 [8, 2], replicated, may hold values from 0 to 7, as said below
- expert_ids: int32 [4096, 8], P('dp'), may hold values from 0 to 15, all different within a row; in each aligned block of 512 rows (0 to 511, 512 to 1023, ...) at most 384 rows name the same one
- gate_weights: float32 [4096, 8], P('dp'), may hold values from 0.05 to 0.5
- expert_weight: bfloat16 [16, 4096, 1024], P('expert'), may hold values from -0.29882812 to 0.29882812
Outputs:
- attended: bfloat16 [4096, 4096], P('dp', 'expert')
- combined: bfloat16 [4096, 1024], P('dp', 'expert')
- row_load: float32 [8], P('dp')
The draws below stay inside these ranges and needn't reach their ends.
Inputs may be any that keep to these rules, and one draw needn't show every extreme that they name: `doc_lengths`: each row's entries are the lengths of its packed documents in order and sum to 512; a zero marks an absent document; some row holds a single document. move_plan[r, 0] is r itself or the row half the dp axis away, (r + 8 / 2) mod 8; a row is handed to its partner only if its pairs in all exceed the partner's, so two partners never both move; move_plan[r, 1] is a block number below 2; at least one row moves a block. `expert_ids`: each token names 8 different experts; among the 512 tokens of one row no expert is named by more than 384 tokens.
All inputs are finite; a program needn't handle non-finite values.
Results may differ from the reference program's by a relative error of at most 0.0095.
Values may be sent and summed in bfloat16 or wider, within the bound.
A program may use at most 128 MiB of HBM per device.

```python
import math
import jax
import jax.numpy as jnp
import numpy as np
from jax import lax

HEADS = 32
HEAD_DIM = 128
QBLOCK = 128
BLOCKS = 4
MAX_DOCS = 8
EXPERT_FF = 1024
EXPERTS = 16
TOPK = 8
ROW_TOKENS = 512
TOKENS = 4096
D_ATT = 4096
CAP = 384
N_DP = 8


def joint_states(key):
    first = jax.random.normal(jax.random.fold_in(key, 11), (TOKENS, D_ATT), jnp.float32)
    second = jax.random.normal(jax.random.fold_in(key, 12), (TOKENS, D_ATT), jnp.float32)
    first = jnp.clip(first, -6.0, 6.0)
    second = jnp.clip(second, -6.0, 6.0)
    return (first, second)


def draw_queries(key, part):
    return joint_states(key)[0].astype(jnp.bfloat16)


def draw_key_states(key, part):
    return joint_states(key)[1].astype(jnp.bfloat16)


def lengths_table(key):
    row_ids = jnp.arange(N_DP, dtype=jnp.int32)
    counts = jax.random.randint(jax.random.fold_in(key, 21), (N_DP, 1), 1, MAX_DOCS + 1)
    single = jax.random.randint(jax.random.fold_in(key, 22), (), 0, N_DP)
    counts = jnp.where(row_ids[:, None] == single, 1, counts)
    raw_cuts = jax.random.randint(jax.random.fold_in(key, 23), (N_DP, MAX_DOCS - 1), 1, ROW_TOKENS)
    used = jnp.arange(MAX_DOCS - 1, dtype=jnp.int32)[None, :] < counts - 1
    cuts = jnp.sort(jnp.where(used, raw_cuts, ROW_TOKENS), axis=1)
    edges = jnp.concatenate([jnp.zeros((N_DP, 1), jnp.int32), cuts.astype(jnp.int32), jnp.full((N_DP, 1), ROW_TOKENS, jnp.int32)], 1)
    return (edges[:, 1:] - edges[:, :-1]).astype(jnp.int32)


def draw_doc_lengths(key, part):
    return lengths_table(key)


def draw_move_plan(key, part):
    lengths = lengths_table(key)
    bounds = jnp.cumsum(lengths, axis=1).astype(jnp.int32)
    positions = jnp.arange(ROW_TOKENS, dtype=jnp.int32)
    starts = jnp.max(jnp.where(bounds[:, None, :] <= positions[None, :, None], bounds[:, None, :], 0), axis=2)
    pairs = (positions[None, :] - starts + 1).reshape(N_DP, BLOCKS, QBLOCK).sum(axis=2)
    totals = jnp.sum(pairs, axis=1)
    row_ids = jnp.arange(N_DP, dtype=jnp.int32)
    partner = (row_ids + N_DP // 2) % N_DP
    moves = totals > totals[partner]
    heavy = jnp.argmax(totals).astype(jnp.int32)
    moves = jnp.where(jnp.any(moves), moves, row_ids == heavy)
    blocks = jnp.argmax(pairs[:, :BLOCKS // 2], axis=1).astype(jnp.int32)
    runner = jnp.where(moves, partner, row_ids)
    return jnp.stack([runner, blocks], 1).astype(jnp.int32)


def shard_levels(own_key, extent, cuts, smallest, largest):
    gain = 1.0
    for axis_at, parts in cuts:
        steps = jax.random.uniform(jax.random.fold_in(jax.random.fold_in(own_key, 6), axis_at), (parts,), jnp.float32, smallest / len(cuts), largest / len(cuts))
        gain = gain * jnp.repeat(jnp.exp(steps), extent[axis_at] // parts).reshape((-1,) + (1,) * (len(extent) - 1 - axis_at))
    return gain


def routed_block(stream_key, own, number, rows, count, top, reach, slope):
    ranking = jax.random.permutation(stream_key, count)
    crowded, usual = portions_of(count, rows * top, reach, slope, True), portions_of(count, rows * top, reach, slope, False)
    places = jnp.arange(count)

    def named(tallies, offset_by):
        used = int((tallies > 0).sum())
        fixed = max(1, used // 4)
        passed = fixed + (places - fixed + offset_by * (used - fixed)) % max(1, count - fixed)
        return jnp.zeros((count,), jnp.int32).at[ranking[jnp.where(places < fixed, places, passed)]].set(jnp.asarray(tallies, jnp.int32))

    tallies = jnp.where(number % 4 == 0, named(crowded, number // 4), named(usual, number - number // 4 - 1))
    mixed = jax.random.permutation(jax.random.fold_in(own, 3), count)
    source_of, receiver = mixed[0:count // 2 * 2:2], mixed[1:count // 2 * 2:2]
    slack = jnp.minimum(tallies[source_of] - 1, reach - tallies[receiver]) // 2
    slack = jnp.where((source_of == ranking[0]) | (receiver == ranking[0]) | (tallies[receiver] == 0), 0, jnp.maximum(slack, 0))
    passed = jax.random.randint(jax.random.fold_in(own, 4), (count // 2,), 0, 1 << 20) % (slack + 1)
    tallies = tallies.at[source_of].add(-passed).at[receiver].add(passed)
    labels = jnp.searchsorted(jnp.cumsum(tallies), jnp.arange(rows * top), side="right").astype(jnp.int32)
    listing = labels.reshape(top, rows).T
    listing = listing[jax.random.permutation(jax.random.fold_in(own, 1), rows)]
    offset_by = jax.random.randint(jax.random.fold_in(own, 2), (rows, 1), 0, top)
    return jnp.take_along_axis(listing, (jnp.arange(top)[None, :] + offset_by) % top, axis=1)


def portions_of(count, total, most, skew, full):
    weights = [(1 << 20) // math.isqrt(grade ** skew) + 1 for grade in range(1, count + 1)]
    largest = most if full else min(most, max(-(-total // count), total * weights[0] // sum(weights)))
    least = 1 if total - largest >= count - 1 else 0
    given, rest = [largest] + [least] * (count - 1), total - largest - least * (count - 1)
    while rest > 0:
        movable = [i for i in range(1, count) if given[i] < largest] or [i for i in range(1, count) if given[i] < most]
        pool, remaining = sum([weights[i] for i in movable]), rest
        for i in movable:
            more = min(most - given[i], max(1, remaining * weights[i] // pool), rest)
            given[i] = given[i] + more
            rest = rest - more
    return np.array(given)


def scatter_about(stream_key, extent, scale, most, cuts=(), kind=jnp.bfloat16):
    entries = jax.random.normal(stream_key, extent, jnp.float32) * scale
    if len(cuts) > 0:
        entries = shard_levels(stream_key, extent, cuts, -0.22, 0.18) * entries
    return jnp.clip(entries, min=-most, max=most).astype(kind)


def setup_inputs(seed: int = 0) -> dict:
    streams_of = jax.random.split(jax.random.key(seed), 9)
    queries = draw_queries(jax.random.fold_in(streams_of[8], 71), 0)
    key_states = draw_key_states(jax.random.fold_in(streams_of[8], 71), 0)
    value_states = scatter_about(streams_of[2], (TOKENS, D_ATT), 1.0, 6.0, ((0, 8), (1, 4)))
    doc_lengths = draw_doc_lengths(jax.random.fold_in(streams_of[8], 71), 0)
    move_plan = draw_move_plan(jax.random.fold_in(streams_of[8], 71), 0)
    expert_ids_keys = jax.random.split(jax.random.fold_in(streams_of[5], 1), TOKENS // ROW_TOKENS)
    expert_ids_turns = jax.random.permutation(jax.random.fold_in(streams_of[5], 3), TOKENS // ROW_TOKENS)
    expert_ids = jax.vmap(lambda own, number: routed_block(jax.random.fold_in(streams_of[5], 2), own, number, ROW_TOKENS, EXPERTS, TOPK, CAP, 1))(expert_ids_keys, expert_ids_turns).reshape((TOKENS, TOPK))
    gate_weights = jnp.clip(0.05 + 0.45 * jax.random.uniform(streams_of[6], (TOKENS, TOPK), jnp.float32) ** shard_levels(streams_of[6], (TOKENS, TOPK), ((0, 8),), -0.2, 0.2), 0.05, 0.5)
    expert_weight = scatter_about(streams_of[7], (EXPERTS, D_ATT, EXPERT_FF), 0.05, 0.29882812, ((0, 4),))
    return dict(queries=queries, key_states=key_states, value_states=value_states, doc_lengths=doc_lengths, move_plan=move_plan, expert_ids=expert_ids, gate_weights=gate_weights, expert_weight=expert_weight)


def token_starts(row_lengths, row_count):
    bounds = jnp.cumsum(row_lengths).astype(jnp.int32)
    positions = jnp.arange(row_count, dtype=jnp.int32)
    return jnp.max(jnp.where(bounds[None, :] <= positions[:, None], bounds[None, :], 0), axis=1)


def attend_row(inputs):
    query_rows, key_rows, value_rows, row_lengths = inputs
    starts = token_starts(row_lengths, ROW_TOKENS)
    positions = jnp.arange(ROW_TOKENS, dtype=jnp.int32)
    query_heads = query_rows.astype(jnp.float32).reshape(ROW_TOKENS, HEADS, HEAD_DIM)
    key_heads = key_rows.astype(jnp.float32).reshape(ROW_TOKENS, HEADS, HEAD_DIM)
    value_heads = value_rows.astype(jnp.float32).reshape(ROW_TOKENS, HEADS, HEAD_DIM)
    scores = jnp.einsum("qhd,khd->hqk", query_heads, key_heads) * (HEAD_DIM ** -0.5)
    allowed = (positions[None, :] <= positions[:, None]) & (positions[None, :] >= starts[:, None])
    scores = jnp.where(allowed[None], scores, -jnp.inf)
    weights = jax.nn.softmax(scores, axis=-1).astype(jnp.bfloat16)
    output = jnp.einsum("hqk,khd->qhd", weights.astype(jnp.float32), value_heads)
    return output.reshape(ROW_TOKENS, D_ATT).astype(jnp.bfloat16)


def reference(queries, key_states, value_states, doc_lengths, move_plan, expert_ids, gate_weights, expert_weight):
    attended = lax.map(attend_row, (queries.reshape(N_DP, ROW_TOKENS, D_ATT), key_states.reshape(N_DP, ROW_TOKENS, D_ATT), value_states.reshape(N_DP, ROW_TOKENS, D_ATT), doc_lengths))
    attended = attended.reshape(TOKENS, D_ATT)

    starts = jax.vmap(lambda lengths_row: token_starts(lengths_row, ROW_TOKENS))(doc_lengths)
    positions = jnp.arange(ROW_TOKENS, dtype=jnp.int32)
    pairs = (positions[None, :] - starts + 1).reshape(N_DP, BLOCKS, QBLOCK).sum(axis=2)
    row_ids = jnp.arange(N_DP, dtype=jnp.int32)
    runner = jnp.where(jnp.arange(BLOCKS, dtype=jnp.int32)[None, :] == move_plan[:, 1:2], move_plan[:, 0:1], row_ids[:, None])
    work = jax.ops.segment_sum(pairs.reshape(-1), runner.reshape(-1).astype(jnp.int32), N_DP)
    row_load = work.astype(jnp.float32) / (QBLOCK * QBLOCK)

    padded = jnp.concatenate([attended, jnp.zeros((1, D_ATT), jnp.bfloat16)], 0)

    def expert_step(carry, expert):
        chosen = expert_ids == expert
        picked = jnp.nonzero(jnp.any(chosen, axis=1), size=CAP * N_DP, fill_value=TOKENS)[0].astype(jnp.int32)
        weight_rows = jnp.sum(jnp.where(chosen, gate_weights, 0.0), axis=1)
        weight_rows = jnp.concatenate([weight_rows, jnp.zeros((1,), weight_rows.dtype)])
        pre_act = jnp.dot(padded[picked], expert_weight[expert], preferred_element_type=jnp.float32)
        rounded = lax.optimization_barrier(jax.nn.silu(pre_act).astype(jnp.bfloat16))
        activated = rounded.astype(jnp.float32)
        return carry.at[picked].add(weight_rows[picked][:, None] * activated), None

    summed, _ = lax.scan(expert_step, jnp.zeros((TOKENS + 1, EXPERT_FF), jnp.float32), jnp.arange(EXPERTS, dtype=jnp.int32))
    combined = summed[:TOKENS].astype(jnp.bfloat16)
    return (attended, combined, row_load)
```

```python
import contextlib
import functools

import jax
import jax.numpy as jnp
from jax import lax
from jax.experimental import pallas as pl
from jax.experimental.pallas import tpu as pltpu
from jax.sharding import PartitionSpec as P

HEAD_DIM = 128
QBLOCK = 128
MESH = pl.DeviceIdType.MESH
LOG2E = 1.4426950408889634
SLOTS = 4


def scope(name):
    return contextlib.nullcontext()


def halves_of(rows):
    return [(0, rows // 2), (rows // 2, rows)]


def bands_of(rows):
    return [(0, rows // 2), (rows // 2, rows * 7 // 8), (rows * 7 // 8, rows)]


def span_pairs(low, high, start, stop):
    first = jnp.maximum(low, start)
    last = jnp.minimum(high, stop)
    count = jnp.maximum(last - first, 0)
    return (count * ((first - start + 1) + (last - start))) // 2


def row_pairs(lens, row, block, docs, row_count):
    low = block * QBLOCK
    total = jnp.int32(0)
    picked = jnp.int32(0)
    edge = jnp.int32(0)
    for doc in range(docs):
        stop = edge + lens[row, doc]
        total = total + span_pairs(0, row_count, edge, stop)
        picked = picked + span_pairs(low, low + QBLOCK, edge, stop)
        edge = stop
    return total, picked


def kernel(dp_size, group, q_hbm, k_hbm, v_hbm, lens_hbm, plan_hbm, ids_hbm, gates_hbm, w_hbm,
           att, comb, load,
           lens, plan, ids, gates, qv, kv, vv, sv, pv, wv, xg, acc, bias, gsc, part, rxd, txx, rxx,
           rx_sem, rd_sem, rf_sem, pr_sem, qr_sem,
           small_sem, in_sem, w_sem, f_sem, sx_sem, sd_sem, sf_sem, ps_sem, qs_sem):
    rows, width = q_hbm.shape
    experts, depth, ff = w_hbm.shape
    f32, bf16 = jnp.float32, jnp.bfloat16
    chips = group // 2
    ck = 2 * HEAD_DIM
    chunks = width // ck
    heads = width // HEAD_DIM
    chip_width = 2 * width
    step = 2 * ck
    owned = ff // group
    columns = 2 * owned
    halves = halves_of(rows)
    bands = bands_of(rows)
    last = len(bands) - 1
    docs = lens.shape[1]
    row = lax.axis_index("dp")
    me = lax.axis_index("expert")
    chip = me // 2
    core = lax.rem(me, 2)
    other = chip * 2 + 1 - core

    def rel(d):
        return lax.rem(chip + d, chips)

    def back(d):
        return lax.rem(chip + chips - d, chips)

    def place(d, c, k):
        if d == 0:
            return k * width + c * ck
        return d * chip_width + c * step + k * ck

    def core_of(k):
        return core if k == 0 else 1 - core

    smalls = ((lens_hbm, lens), (plan_hbm, plan), (ids_hbm, ids), (gates_hbm, gates))

    def small_copy(i):
        return pltpu.make_async_copy(*smalls[i], small_sem.at[i])

    def in_copies(p, c):
        lo, hi = halves[p]
        cols = pl.ds(c * ck, ck)
        copies = [
            pltpu.make_async_copy(src.at[lo:hi, cols], dst.at[lo:hi, cols], in_sem.at[p, c, i])
            for i, (src, dst) in enumerate(((q_hbm, qv), (k_hbm, kv)))
        ]
        for i in range(2):
            h = 2 * c + i
            copies.append(pltpu.make_async_copy(
                v_hbm.at[lo:hi, pl.ds(h * HEAD_DIM, HEAD_DIM)],
                vv.at[h, lo:hi, pl.ds(0, HEAD_DIM)], in_sem.at[p, c, 2 + i]))
        return copies

    def cols_from(j):
        return pl.ds(pl.multiple_of(rel(j) * columns, 128), columns)

    def own_weight(e, k, j):
        return pltpu.make_async_copy(
            w_hbm.at[e, pl.ds(pl.multiple_of((chip * 2 + core_of(k)) * width, 128), width),
                     cols_from(j)],
            wv.at[e, pl.ds(k * width, width), pl.ds(j * columns, columns)],
            w_sem.at[e, k, j])

    def far_weight(e, d, c, k, j):
        return pltpu.make_async_copy(
            w_hbm.at[e, pl.ds(pl.multiple_of(
                (back(d) * 2 + core_of(k)) * width + c * ck, 128), ck), cols_from(j)],
            wv.at[e, pl.ds(place(d, c, k), ck), pl.ds(j * columns, columns)],
            f_sem.at[e, d - 1, c, k, j])

    quarters = [(k, j) for k in range(2) for j in range(chips)]

    def cross_copy(b, c, d):
        lo, hi = bands[b]
        return pltpu.make_async_remote_copy(
            src_ref=xg.at[lo:hi, pl.ds(place(0, c, 0), ck)],
            dst_ref=xg.at[lo:hi, pl.ds(place(d, c, 0), ck)],
            send_sem=sx_sem.at[d - 1, b, c], recv_sem=rx_sem.at[d - 1, b, c],
            device_id={"expert": rel(d) * 2 + core}, device_id_type=MESH)

    def side_copy(p, c):
        lo, hi = halves[p]
        return pltpu.make_async_remote_copy(
            src_ref=xg.at[lo:hi, pl.ds(place(0, c, 0), ck)],
            dst_ref=xg.at[lo:hi, pl.ds(place(0, c, 1), ck)],
            send_sem=sd_sem.at[p, c], recv_sem=rd_sem.at[p, c],
            device_id={"expert": other}, device_id_type=MESH)

    def pass_copy(b, c, d):
        lo, hi = bands[b]
        return pltpu.make_async_remote_copy(
            src_ref=xg.at[lo:hi, pl.ds(place(d, c, 0), ck)],
            dst_ref=xg.at[lo:hi, pl.ds(place(d, c, 1), ck)],
            send_sem=sf_sem.at[d - 1, b, c], recv_sem=rf_sem.at[d - 1, b, c],
            device_id={"expert": other}, device_id_type=MESH)

    def pair_copy(b, d):
        lo, hi = bands[b]
        return pltpu.make_async_remote_copy(
            src_ref=part.at[d * 2 + 1 - core, lo:hi], dst_ref=rxd.at[d, lo:hi],
            send_sem=ps_sem.at[b, d], recv_sem=pr_sem.at[b, d],
            device_id={"expert": other}, device_id_type=MESH)

    def sum_copy(b, d):
        lo, hi = bands[b]
        return pltpu.make_async_remote_copy(
            src_ref=txx.at[d - 1, lo:hi], dst_ref=rxx.at[d - 1, lo:hi],
            send_sem=qs_sem.at[b, d - 1], recv_sem=qr_sem.at[b, d - 1],
            device_id={"expert": rel(d) * 2 + core}, device_id_type=MESH)

    small_copy(0).start()
    for p in range(2):
        for c in range(chunks):
            for copy in in_copies(p, c):
                copy.start()
    for i in range(1, 4):
        small_copy(i).start()

    barrier = pltpu.get_barrier_semaphore()
    pl.semaphore_signal(barrier, inc=1, device_id={"expert": other}, device_id_type=MESH)
    for d in range(1, chips):
        pl.semaphore_signal(
            barrier, inc=1, device_id={"expert": rel(d) * 2 + core}, device_id_type=MESH)

    for h in range(heads):
        vv[h, :, HEAD_DIM:] = jnp.ones((rows, HEAD_DIM), bf16)

    with scope("lenswait"):
        small_copy(0).wait()

    def set_bias(p):
        lo, hi = halves[p]
        pos = lax.broadcasted_iota(jnp.int32, (hi - lo, hi), 0) + lo
        key_pos = lax.broadcasted_iota(jnp.int32, (hi - lo, hi), 1)
        column = lax.broadcasted_iota(jnp.int32, (hi - lo, 1), 0) + lo
        starts = jnp.zeros((hi - lo, 1), jnp.int32)
        edge = jnp.int32(0)
        for doc in range(docs):
            edge = edge + lens[row, doc]
            starts = jnp.where(column >= edge, jnp.maximum(starts, edge), starts)
        bias[lo:hi, :hi] = jnp.where((key_pos <= pos) & (key_pos >= starts), 0.0, -1e30)

    set_bias(0)

    scale = HEAD_DIM ** -0.5 * LOG2E
    units = [(p, h) for p in range(2) for h in range(heads)]

    def score(u):
        p, h = units[u]
        lo, hi = halves[p]
        cols = slice(h * HEAD_DIM, (h + 1) * HEAD_DIM)
        s = lax.dot_general(qv[lo:hi, cols], kv[:hi, cols], (((1,), (1,)), ((), ())),
                            preferred_element_type=f32)
        sv[u % SLOTS, :hi - lo, :hi] = s + bias[lo:hi, :hi]

    def soften(u):
        p, h = units[u]
        lo, hi = halves[p]
        s = sv[u % SLOTS, :hi - lo, :hi]
        top = jnp.max(s, axis=1, keepdims=True)
        pv[u % SLOTS, :hi - lo, :hi] = jnp.exp2((s - top) * scale).astype(bf16)

    def mix(u):
        p, h = units[u]
        lo, hi = halves[p]
        o = jnp.dot(pv[u % SLOTS, :hi - lo, :hi], vv[h, :hi, :], preferred_element_type=f32)
        o = (o[:, :HEAD_DIM] / o[:, HEAD_DIM:]).astype(bf16)
        xg[lo:hi, h * HEAD_DIM:(h + 1) * HEAD_DIM] = o
        att[lo:hi, h * HEAD_DIM:(h + 1) * HEAD_DIM] = o

    def send(p, c):
        if p == 0 and c == 0:
            with scope("barwait"):
                pl.semaphore_wait(barrier, chips)
        for b in range(len(bands)):
            if bands[b][0] == halves[p][0]:
                for d in range(1, chips):
                    cross_copy(b, c, d).start()
        side_copy(p, c).start()

    own_starts = [(e, k, j) for e in range(experts) for k, j in quarters]
    far_starts = [(e, d, c, k, j) for c in range(chunks) for d in range(1, chips)
                  for e in range(experts) for k, j in quarters]
    started = [0]

    def start_own(n):
        for at in own_starts[started[0]:started[0] + n]:
            own_weight(*at).start()
        started[0] += n

    def arrive_inputs(u):
        p, h = units[u]
        if h % 2 == 0:
            with scope("inwait"):
                for copy in in_copies(p, h // 2):
                    copy.wait()

    with scope("attend"):
        count = len(units)
        for u in range(2):
            arrive_inputs(u)
            score(u)
        for u in range(2):
            soften(u)
        for u in range(2):
            mix(u)
        send(0, 0)
        for t in range(2, count + 2):
            if t < count:
                if units[t] == (1, 0):
                    set_bias(1)
                arrive_inputs(t)
                score(t)
            if 2 < t < count + 1:
                soften(t - 1)
            if 3 < t:
                mix(t - 2)
                p, h = units[t - 2]
                if h % 2 == 1:
                    send(p, h // 2)
                start_own(-(-len(own_starts) // (count - 2)))
        start_own(len(own_starts))
        for b in range(len(bands)):
            if bands[b][0] not in [lo for lo, _ in halves]:
                for c in range(chunks):
                    for d in range(1, chips):
                        cross_copy(b, c, d).start()

    with scope("startfar"):
        for at in far_starts:
            far_weight(*at).start()

    arrivals = [(b, c, d) for b in range(len(bands)) for c in range(chunks)
                for d in range(1, chips)]
    sent = [0]

    def forward(b, c, d):
        upto = arrivals.index((b, c, d)) + 1
        while sent[0] < upto:
            with scope("fwdwait"):
                cross_copy(*arrivals[sent[0]]).wait_recv()
            pass_copy(*arrivals[sent[0]]).start()
            sent[0] += 1

    def forward_more(n):
        if n > 0:
            forward(*arrivals[min(sent[0] + n, len(arrivals)) - 1])

    def set_gates(e):
        chosen = ids[...] == me * experts + e
        line = jnp.sum(jnp.where(chosen, gates[...], 0.0), axis=0, keepdims=True)
        for r in range(0, rows, 128):
            gsc[e, r:r + 128, :] = jnp.broadcast_to(line[:, r:r + 128], (128, 128)).T

    for i in range(1, 4):
        small_copy(i).wait()
    for e in range(experts):
        with scope("wownwait"):
            for k, j in quarters:
                own_weight(e, k, j).wait()
        with scope("near"):
            set_gates(e)
            if e == 0:
                acc[e] = jnp.dot(xg[:, :width], wv[e, :width, :], preferred_element_type=f32)
                with scope("sidewait"):
                    for p in range(2):
                        for c in range(chunks):
                            side_copy(p, c).wait_recv()
                acc[e] += jnp.dot(xg[:, width:chip_width], wv[e, width:chip_width, :],
                                  preferred_element_type=f32)
            else:
                acc[e] = jnp.dot(xg[:, :chip_width], wv[e, :chip_width, :],
                                 preferred_element_type=f32)
        if e < experts - 1:
            forward_more(min(1, chunks * (chips - 1) - sent[0]))

    with scope("misc"):
        partner = lax.rem(row + dp_size // 2, dp_size)
        own_total, own_moved = row_pairs(lens, row, plan[1, row], docs, rows)
        _, their_moved = row_pairs(lens, partner, plan[1, partner], docs, rows)
        work = own_total - jnp.where(plan[0, row] != row, own_moved, 0)
        work = work + jnp.where(plan[0, partner] != partner, their_moved, 0)
        load[...] = jnp.full((1,), work.astype(f32) * (1.0 / (QBLOCK * QBLOCK)))

    def arrive(b, c, d):
        forward(b, c, d)
        with scope("passwait"):
            pass_copy(b, c, d).wait_recv()
        far_ready(b, c, d)

    def far_ready(b, c, d):
        if b == 0:
            for e in range(experts):
                for k, j in quarters:
                    far_weight(e, d, c, k, j).wait()

    def add_far(b, span):
        lo, hi = bands[b]
        for e in range(experts):
            acc[e, lo:hi, :] += jnp.dot(xg[lo:hi, span], wv[e, span, :],
                                        preferred_element_type=f32)

    rt = 32
    tile = max(owned, 128)

    def close(b, span):
        lo, hi = bands[b]
        for j in list(range(1, chips)) + [0]:
            for at in range(j * columns, (j + 1) * columns, tile):
                cols = slice(at, at + tile)
                for e in range(experts):
                    acc[e, lo:hi, cols] += jnp.dot(xg[lo:hi, span], wv[e, span, cols],
                                                   preferred_element_type=f32)
                for r in range(lo, hi, rt):
                    total = jnp.zeros((rt, tile), f32)
                    for e in range(experts):
                        h = acc[e, r:r + rt, cols] * 0.5
                        total = total + (h * jnp.tanh(h) + h) * jnp.concatenate(
                            [gsc[e, r:r + rt, :]] * (tile // 128), axis=1)
                    total = total.astype(bf16)
                    for i in range(tile // owned):
                        part[at // owned + i, r:r + rt, :] = total[:, i * owned:(i + 1) * owned]
            pair_copy(b, j).start()

    def exchange(b):
        lo, hi = bands[b]
        for d in range(1, chips):
            with scope("pairwait"):
                pair_copy(b, d).wait_recv()
            txx[d - 1, lo:hi, :] = (part[d * 2 + core, lo:hi, :].astype(f32)
                                    + rxd[d, lo:hi, :].astype(f32)).astype(bf16)
            sum_copy(b, d).start()

    def finish(b):
        lo, hi = bands[b]
        with scope("pairwait"):
            pair_copy(b, 0).wait_recv()
        total = part[core, lo:hi, :].astype(f32) + rxd[0, lo:hi, :].astype(f32)
        for d in range(1, chips):
            with scope("sumwait"):
                sum_copy(b, d).wait_recv()
            total = total + rxx[d - 1, lo:hi, :].astype(f32)
        comb[lo:hi, :] = total.astype(bf16)

    steps = [(c, d) for c in range(chunks) for d in range(1, chips)]
    for b in range(len(bands)):
        for i, (c, d) in enumerate(steps[:-1]):
            forward(b, *steps[i + 1])
            arrive(b, c, d)
            with scope(f"far{b}"):
                add_far(b, slice(place(d, c, 0), place(d, c, 0) + step))
            if b > 0 and i == len(steps) // 2:
                exchange(b - 1)
        if b > 0 and len(steps) == 1:
            exchange(b - 1)
        c, d = steps[-1]
        forward(b, c, d)
        if b < last:
            forward(b + 1, *steps[0])
        far_ready(b, c, d)
        with scope(f"half{b}"):
            add_far(b, slice(place(d, c, 0), place(d, c, 0) + ck))
        with scope("passwait"):
            pass_copy(b, c, d).wait_recv()
        with scope(f"close{b}"):
            close(b, slice(place(d, c, 1), place(d, c, 1) + ck))
    exchange(last)
    with scope("finish"):
        for b in range(len(bands)):
            finish(b)

    with scope("endside"):
        for p in range(2):
            for c in range(chunks):
                side_copy(p, c).wait_send()
    with scope("endcross"):
        for b, c, d in arrivals:
            cross_copy(b, c, d).wait_send()
    with scope("endpass"):
        for b, c, d in arrivals:
            pass_copy(b, c, d).wait_send()
    with scope("endsum"):
        for b in range(len(bands)):
            for d in range(chips):
                pair_copy(b, d).wait_send()
            for d in range(1, chips):
                sum_copy(b, d).wait_send()


def emit(att, comb, load, att_hbm, comb_hbm, load_hbm, sem):
    copies = [pltpu.make_async_copy(src, dst, sem.at[i]) for i, (src, dst) in enumerate(
        ((att, att_hbm), (comb, comb_hbm), (load, load_hbm)))]
    for copy in copies:
        copy.start()
    for copy in copies:
        copy.wait()


def shards(dp_size, group, queries, key_states, value_states, doc_lengths, move_plan,
           expert_ids, gate_weights, expert_weight):
    rows, width = queries.shape
    experts, depth, ff = expert_weight.shape
    topk = expert_ids.shape[1]
    chips = group // 2
    chunks = width // (2 * HEAD_DIM)
    heads = width // HEAD_DIM
    owned = ff // group
    half = rows // 2
    nb = len(bands_of(rows))
    bf16, f32, i32 = jnp.bfloat16, jnp.float32, jnp.int32
    hbm = pl.BlockSpec(memory_space=pl.ANY)
    vmem = pl.BlockSpec(memory_space=pltpu.VMEM)
    dma = pltpu.SemaphoreType.DMA
    local = [
        dma((4,)),
        dma((2, chunks, 4)),
        dma((experts, 2, chips)),
        dma((experts, chips - 1, chunks, 2, chips)),
        dma((chips - 1, nb, chunks)),
        dma((2, chunks)),
        dma((chips - 1, nb, chunks)),
        dma((nb, chips)),
        dma((nb, chips - 1)),
    ]

    def scoped(*refs):
        pl.run_scoped(functools.partial(kernel, dp_size, group, *refs), *local)

    outs = pl.pallas_call(
        scoped,
        out_shape=(
            pltpu.VMEM((rows, width), bf16),
            pltpu.VMEM((rows, owned), bf16),
            pltpu.VMEM((1,), f32),
        ),
        in_specs=[hbm] * 8,
        out_specs=(vmem, vmem, vmem),
        scratch_shapes=[
            pltpu.SMEM(doc_lengths.shape, i32),
            pltpu.SMEM(move_plan.shape[::-1], i32),
            pltpu.VMEM((topk, rows), i32),
            pltpu.VMEM((topk, rows), f32),
            pltpu.VMEM((rows, width), bf16),
            pltpu.VMEM((rows, width), bf16),
            pltpu.VMEM((heads, rows, 2 * HEAD_DIM), bf16),
            pltpu.VMEM((SLOTS, half, rows), f32),
            pltpu.VMEM((SLOTS, half, rows), bf16),
            pltpu.VMEM((experts, depth, ff), bf16),
            pltpu.VMEM((rows, depth), bf16),
            pltpu.VMEM((experts, rows, ff), f32),
            pltpu.VMEM((rows, rows), f32),
            pltpu.VMEM((experts, rows, 128), f32),
            pltpu.VMEM((group, rows, owned), bf16),
            pltpu.VMEM((chips, rows, owned), bf16),
            pltpu.VMEM((chips - 1, rows, owned), bf16),
            pltpu.VMEM((chips - 1, rows, owned), bf16),
            dma((chips - 1, nb, chunks)),
            dma((2, chunks)),
            dma((chips - 1, nb, chunks)),
            dma((nb, chips)),
            dma((nb, chips - 1)),
        ],
        compiler_params=pltpu.CompilerParams(
            collective_id=0, has_side_effects=True, vmem_limit_bytes=64_000_000),
    )(queries, key_states, value_states, doc_lengths, move_plan.T, expert_ids.T,
      gate_weights.T, expert_weight)
    return pl.pallas_call(
        emit,
        out_shape=(
            jax.ShapeDtypeStruct((rows, width), bf16),
            jax.ShapeDtypeStruct((rows, owned), bf16),
            jax.ShapeDtypeStruct((1,), f32),
        ),
        in_specs=[vmem, vmem, vmem],
        out_specs=(hbm, hbm, hbm),
        scratch_shapes=[dma((3,))],
    )(*[pltpu.with_memory_space_constraint(out, pltpu.VMEM) for out in outs])


def solution(mesh):
    in_specs = (
        P("dp", "expert"),
        P("dp", "expert"),
        P("dp", "expert"),
        P(),
        P(),
        P("dp", None),
        P("dp", None),
        P("expert", None, None),
    )
    out_specs = (P("dp", "expert"), P("dp", "expert"), P("dp"))
    body = functools.partial(shards, mesh.shape["dp"], mesh.shape["expert"])
    return jax.shard_map(body, mesh=mesh, in_specs=in_specs, out_specs=out_specs, check_vma=False)
```
